64 devices in a mesh: dp: 4 (over x, y), tp: 16 (over z, core).
Axes of the slice: x: 2, y: 2, z: 8, core: 2. Of those that a mesh axis runs over, the one named last changes fastest.
The devices are a block of a 4x4x8 slice.
Arguments:
- y_one: float32 [64, 256, 1024], P('dp', 'tp'), parts along dimension 0
- y_two: float32 [64, 256, 1024], P('dp', 'tp'), parts along dimension 0
- dy_one: float32 [64, 256, 1024], P('dp', 'tp'), parts along dimension 0
- dy_two: float32 [64, 256, 1024], P('dp', 'tp'), parts along dimension 0
- w_qkv: bfloat16 [1, 1024, 16, 3, 64], P(None, None, 'tp')
- w_out: bfloat16 [1, 16, 64, 1024], P(None, 'tp')
- w_up: bfloat16 [1, 1024, 4096], P(None, None, 'tp')
- w_down: bfloat16 [1, 4096, 1024], P(None, 'tp')
Outputs:
- output 1: float32 [64, 256, 1024], P('dp', 'tp'), parts along dimension 0
- output 2: float32 [64, 256, 1024], P('dp', 'tp'), parts along dimension 0
- output 3: float32 [64, 256, 1024], P('dp', 'tp'), parts along dimension 0
- output 4: float32 [64, 256, 1024], P('dp', 'tp'), parts along dimension 0
- output 5: float32 [4, 1024, 16, 3, 64], P('dp', None, 'tp'), parts along dimension 0
- output 6: float32 [4, 16, 64, 1024], P('dp', 'tp'), parts along dimension 0
- output 7: float32 [4, 1024, 4096], P('dp', None, 'tp'), parts along dimension 0
- output 8: float32 [4, 4096, 1024], P('dp', 'tp'), parts along dimension 0
There are 4 independent parts. The reference program is written for one: setup_inputs(seed, part) draws one part's arguments, and reference() takes and returns one part's arrays. A program takes and returns all parts, laid end to end along the dimension named above; an argument that names none is the same for every part.
All inputs are finite; a program needn't handle non-finite values.
Results may differ from the reference program's by a relative error of at most 0.00846033.
Values are sent between devices in bfloat16 or wider.
A program may use at most 768 MiB of HBM per device.

```python
import jax
import jax.numpy as jnp
from jax import lax

SEQ_COUNT = 16
SEQ_LEN = 256
HIDDEN = 1024
N_HEADS = 16
FFN_DIM = 4096
N_LAYERS = 1

HEAD_DIM = HIDDEN // N_HEADS
TOKENS = SEQ_COUNT * SEQ_LEN
STATE_SHAPE = (SEQ_COUNT, SEQ_LEN, HIDDEN)
RMS_EPS = 1e-6
ATTN_SCALE = HEAD_DIM ** -0.5
Q_GAIN = 2.5
OUT_GAIN = 0.6
DOWN_GAIN = 0.5


def setup_inputs(seed: int = 0, part: int = 0) -> dict:
    base_key = jax.random.key(seed)
    act_keys = jax.random.split(jax.random.fold_in(base_key, part), 4)
    w_keys = jax.random.split(jax.random.fold_in(base_key, 100003), 4)
    y_one = jax.random.normal(act_keys[0], STATE_SHAPE, jnp.float32)
    y_two = jax.random.normal(act_keys[1], STATE_SHAPE, jnp.float32)
    dy_one = jax.random.normal(act_keys[2], STATE_SHAPE, jnp.float32)
    dy_two = jax.random.normal(act_keys[3], STATE_SHAPE, jnp.float32)
    qkv_gain = jnp.array([Q_GAIN, 1.0, 1.0], jnp.float32).reshape(1, 1, 1, 3, 1)
    w_qkv = (jax.random.normal(w_keys[0], (N_LAYERS, HIDDEN, N_HEADS, 3, HEAD_DIM), jnp.float32) * qkv_gain * HIDDEN ** -0.5).astype(jnp.bfloat16)
    w_out = (jax.random.normal(w_keys[1], (N_LAYERS, N_HEADS, HEAD_DIM, HIDDEN), jnp.float32) * (OUT_GAIN * HIDDEN ** -0.5)).astype(jnp.bfloat16)
    w_up = (jax.random.normal(w_keys[2], (N_LAYERS, HIDDEN, FFN_DIM), jnp.float32) * HIDDEN ** -0.5).astype(jnp.bfloat16)
    w_down = (jax.random.normal(w_keys[3], (N_LAYERS, FFN_DIM, HIDDEN), jnp.float32) * (DOWN_GAIN * FFN_DIM ** -0.5)).astype(jnp.bfloat16)
    return {"y_one": y_one, "y_two": y_two, "dy_one": dy_one, "dy_two": dy_two, "w_qkv": w_qkv, "w_out": w_out, "w_up": w_up, "w_down": w_down}


def rms_norm(tensor):
    return tensor * lax.rsqrt(jnp.mean(tensor * tensor, axis=-1, keepdims=True) + RMS_EPS)


def rms_back(tensor, grad_in):
    inv_rms = lax.rsqrt(jnp.mean(tensor * tensor, axis=-1, keepdims=True) + RMS_EPS)
    return inv_rms * grad_in - tensor * (inv_rms * inv_rms * inv_rms) * jnp.mean(grad_in * tensor, axis=-1, keepdims=True)


def gelu_tanh(tensor):
    return jax.nn.gelu(tensor, approximate=True)


def mixed_dot(left, right):
    return jnp.dot(left, right, preferred_element_type=jnp.float32)


def as_wide(tensor):
    return tensor.astype(jnp.float32)


def attn_forward(qkv_seq):
    q_heads = as_wide(qkv_seq[0])
    k_heads = as_wide(qkv_seq[1])
    v_heads = as_wide(qkv_seq[2])
    scores = jnp.einsum("nqd,nkd->nqk", q_heads, k_heads) * ATTN_SCALE
    attn_prob = jax.nn.softmax(scores, axis=-1)
    context = jnp.einsum("nqk,nkd->nqd", as_wide(attn_prob.astype(jnp.bfloat16)), v_heads)
    return context.astype(jnp.bfloat16)


def attn_backward(operands):
    qkv_seq, d_context = operands
    q_heads = as_wide(qkv_seq[0])
    k_heads = as_wide(qkv_seq[1])
    v_heads = as_wide(qkv_seq[2])
    scores = jnp.einsum("nqd,nkd->nqk", q_heads, k_heads) * ATTN_SCALE
    attn_prob = jax.nn.softmax(scores, axis=-1)
    d_ctx = as_wide(d_context)
    d_prob = jnp.einsum("nqd,nkd->nqk", d_ctx, v_heads)
    d_value = jnp.einsum("nqk,nqd->nkd", as_wide(attn_prob.astype(jnp.bfloat16)), d_ctx)
    d_scores = attn_prob * (d_prob - jnp.sum(d_prob * attn_prob, axis=-1, keepdims=True)) * ATTN_SCALE
    d_scores = as_wide(d_scores.astype(jnp.bfloat16))
    d_query = jnp.einsum("nqk,nkd->nqd", d_scores, k_heads)
    d_key = jnp.einsum("nqk,nqd->nkd", d_scores, q_heads)
    return jnp.stack([d_query, d_key, d_value]).astype(jnp.bfloat16)


def block_backward(state_in, layer_weights):
    y_one, y_two, dy_one, dy_two = state_in
    w_qkv, w_out, w_up, w_down = layer_weights
    w_qkv_flat = w_qkv.reshape(HIDDEN, 3 * HIDDEN)
    w_out_flat = w_out.reshape(HIDDEN, HIDDEN)
    u_mlp = rms_norm(y_one).astype(jnp.bfloat16).reshape(TOKENS, HIDDEN)
    pre_act = mixed_dot(u_mlp, w_up)
    hidden, gelu_pull = jax.vjp(gelu_tanh, pre_act)
    hidden_b = hidden.astype(jnp.bfloat16)
    x_two = y_two - mixed_dot(hidden_b, w_down).reshape(STATE_SHAPE)
    cot_mlp = dy_two.astype(jnp.bfloat16).reshape(TOKENS, HIDDEN)
    dw_down = mixed_dot(hidden_b.T, cot_mlp)
    d_pre = gelu_pull(mixed_dot(cot_mlp, w_down.T))[0].astype(jnp.bfloat16)
    dw_up = mixed_dot(u_mlp.T, d_pre)
    dy_one = dy_one + rms_back(y_one, mixed_dot(d_pre, w_up.T).reshape(STATE_SHAPE))
    u_att = rms_norm(x_two).astype(jnp.bfloat16).reshape(TOKENS, HIDDEN)
    qkv_seqs = mixed_dot(u_att, w_qkv_flat).astype(jnp.bfloat16).reshape(SEQ_COUNT, SEQ_LEN, N_HEADS, 3, HEAD_DIM).transpose(0, 3, 2, 1, 4)
    context = lax.map(attn_forward, qkv_seqs)
    context_flat = context.transpose(0, 2, 1, 3).reshape(TOKENS, HIDDEN)
    x_one = y_one - mixed_dot(context_flat, w_out_flat).reshape(STATE_SHAPE)
    cot_att = dy_one.astype(jnp.bfloat16).reshape(TOKENS, HIDDEN)
    dw_out = mixed_dot(context_flat.T, cot_att)
    d_context = mixed_dot(cot_att, w_out_flat.T).astype(jnp.bfloat16).reshape(SEQ_COUNT, SEQ_LEN, N_HEADS, HEAD_DIM).transpose(0, 2, 1, 3)
    d_qkv = lax.map(attn_backward, (qkv_seqs, d_context))
    d_qkv_flat = d_qkv.transpose(0, 3, 2, 1, 4).reshape(TOKENS, 3 * HIDDEN)
    dw_qkv = mixed_dot(u_att.T, d_qkv_flat)
    dx_two = dy_two + rms_back(x_two, mixed_dot(d_qkv_flat, w_qkv_flat.T).reshape(STATE_SHAPE))
    grads = (dw_qkv.reshape(HIDDEN, N_HEADS, 3, HEAD_DIM), dw_out.reshape(N_HEADS, HEAD_DIM, HIDDEN), dw_up, dw_down)
    return (x_one, x_two, dy_one, dx_two), grads


def reference(y_one, y_two, dy_one, dy_two, w_qkv, w_out, w_up, w_down):
    final_state, grad_stack = lax.scan(block_backward, (y_one, y_two, dy_one, dy_two), (w_qkv, w_out, w_up, w_down), reverse=True)
    x_one, x_two, dx_one, dx_two = final_state
    dw_qkv, dw_out, dw_up, dw_down = grad_stack
    return (x_one, x_two, dx_one, dx_two, dw_qkv, dw_out, dw_up, dw_down)
```

```python
import jax
import jax.numpy as jnp
from jax import lax
from jax.sharding import PartitionSpec as P

RMS_EPS = 1e-6


def rms_norm(tensor):
    return tensor * lax.rsqrt(jnp.mean(tensor * tensor, axis=-1, keepdims=True) + RMS_EPS)


def rms_back(tensor, grad_in):
    inv_rms = lax.rsqrt(jnp.mean(tensor * tensor, axis=-1, keepdims=True) + RMS_EPS)
    return inv_rms * grad_in - tensor * (inv_rms * inv_rms * inv_rms) * jnp.mean(grad_in * tensor, axis=-1, keepdims=True)


def gelu_tanh(tensor):
    return jax.nn.gelu(tensor, approximate=True)


def gather(tensor):
    return lax.all_gather(tensor, "tp", axis=0, tiled=False)


def dot32(spec, left, right):
    return jnp.einsum(spec, left, right, preferred_element_type=jnp.float32)


def layer_backward(y_one, y_two, dy_one, dy_two, wq, wo, wu, wd):
    seqs, own, hidden = y_one.shape
    n_loc, dim = wo.shape[0], wo.shape[1]
    attn_scale = dim ** -0.5
    toks = seqs * own
    flat = lambda t: t.reshape(toks, hidden)

    u_mlp = flat(rms_norm(y_one).astype(jnp.bfloat16))
    cot_mlp = flat(dy_two.astype(jnp.bfloat16))
    wu_all = gather(wu)
    wd_all = gather(wd)
    u_all = gather(u_mlp)
    c_all = gather(cot_mlp)
    wq_all = gather(wq.reshape(hidden, n_loc * 3 * dim).T)
    wo_all = gather(wo.reshape(n_loc * dim, hidden))

    pre = dot32("tk,dkf->dtf", u_mlp, wu_all)
    hid, pull = jax.vjp(gelu_tanh, pre)
    g_out = dot32("dtf,dfh->th", hid.astype(jnp.bfloat16), wd_all)
    x_two = y_two - g_out.reshape(y_two.shape)
    d_pre = pull(dot32("th,dfh->dtf", cot_mlp, wd_all))[0].astype(jnp.bfloat16)
    du_mlp = dot32("dtf,dkf->tk", d_pre, wu_all)
    dy_one = dy_one + rms_back(y_one, du_mlp.reshape(y_one.shape))

    u_att = rms_norm(x_two).astype(jnp.bfloat16)
    cot_att = dy_one.astype(jnp.bfloat16)
    ua_all = gather(flat(u_att))
    ca_all = gather(flat(cot_att))
    n_dev = ua_all.shape[0]
    every = n_dev * toks

    u_all = u_all.reshape(every, hidden)
    c_all = c_all.reshape(every, hidden)
    pre_c = dot32("tk,kf->tf", u_all, wu)
    hid_c, pull_c = jax.vjp(gelu_tanh, pre_c)
    g_down = dot32("tf,th->fh", hid_c.astype(jnp.bfloat16), c_all)
    d_pre_c = pull_c(dot32("th,fh->tf", c_all, wd))[0].astype(jnp.bfloat16)
    g_up = dot32("tk,tf->kf", u_all, d_pre_c)

    ua_all = ua_all.reshape(every, hidden)
    ca_all = ca_all.reshape(every, hidden)

    def by_seq(t, width):
        return t.reshape(n_dev, seqs, own, n_loc, width).transpose(1, 3, 0, 2, 4).reshape(seqs, n_loc, n_dev * own, width)

    def by_dev(t):
        return t.reshape(seqs, n_loc, n_dev, own, dim).transpose(2, 0, 3, 1, 4).reshape(n_dev, toks, n_loc, dim)

    qkv = [by_seq(dot32("th,hc->tc", ua_all, wq[:, :, j].reshape(hidden, n_loc * dim)).astype(jnp.bfloat16), dim) for j in range(3)]
    q, k, v = qkv
    d_ctx = by_seq(dot32("th,ch->tc", ca_all, wo.reshape(n_loc * dim, hidden)).astype(jnp.bfloat16), dim)
    scores = dot32("bnqd,bnkd->bnqk", q, k) * attn_scale
    prob = jax.nn.softmax(scores, axis=-1)
    prob_b = prob.astype(jnp.bfloat16)
    ctx = dot32("bnqk,bnkd->bnqd", prob_b, v).astype(jnp.bfloat16)
    d_prob = dot32("bnqd,bnkd->bnqk", d_ctx, v)
    d_v = dot32("bnqk,bnqd->bnkd", prob_b, d_ctx).astype(jnp.bfloat16)
    d_s = (prob * (d_prob - jnp.sum(d_prob * prob, axis=-1, keepdims=True)) * attn_scale).astype(jnp.bfloat16)
    d_q = dot32("bnqk,bnkd->bnqd", d_s, k).astype(jnp.bfloat16)
    d_k = dot32("bnqk,bnqd->bnkd", d_s, q).astype(jnp.bfloat16)

    mine = jnp.stack([by_dev(t) for t in (ctx, d_q, d_k, d_v)], axis=3)
    c_head = mine[:, :, :, 0].reshape(every, n_loc * dim)
    d_head = mine[:, :, :, 1:].reshape(every, n_loc * 3 * dim)
    g_out_w = dot32("tc,th->ch", c_head, ca_all)
    g_qkv = dot32("th,tc->hc", ua_all, d_head)
    packed = lax.all_to_all(mine.reshape(n_dev, toks, n_loc * 4 * dim), "tp", 0, 0, tiled=False)
    packed = packed.reshape(n_dev, toks, n_loc, 4, dim)
    c_tok = packed[:, :, :, 0].reshape(n_dev, toks, n_loc * dim)
    d_tok = packed[:, :, :, 1:].reshape(n_dev, toks, n_loc * 3 * dim)
    f_out = dot32("dtc,dch->th", c_tok, wo_all)
    x_one = y_one - f_out.reshape(y_one.shape)
    du_att = dot32("dtc,dch->th", d_tok, wq_all)
    dx_two = dy_two + rms_back(x_two, du_att.reshape(x_two.shape))
    return x_one, x_two, dy_one, dx_two, g_qkv.reshape(wq.shape), g_out_w.reshape(wo.shape), g_up, g_down


def local_backward(y_one, y_two, dy_one, dy_two, w_qkv, w_out, w_up, w_down):
    grads = []
    state = (y_one, y_two, dy_one, dy_two)
    for idx in reversed(range(w_qkv.shape[0])):
        res = layer_backward(*state, w_qkv[idx], w_out[idx], w_up[idx], w_down[idx])
        state = res[:4]
        grads.append(res[4:])
    return state + tuple(jnp.stack(g[::-1]) for g in zip(*grads))


def solution(mesh):
    state_spec = P("dp", "tp", None)
    in_specs = (state_spec, state_spec, state_spec, state_spec, P(None, None, "tp", None, None), P(None, "tp", None, None), P(None, None, "tp"), P(None, "tp", None))
    out_specs = (state_spec, state_spec, state_spec, state_spec, P("dp", None, "tp", None, None), P("dp", "tp", None, None), P("dp", None, "tp"), P("dp", "tp", None))
    return jax.shard_map(local_backward, mesh=mesh, in_specs=in_specs, out_specs=out_specs, check_vma=False)
```

```python
import functools

import jax
import jax.numpy as jnp
from jax import lax
from jax.experimental import pallas as pl
from jax.experimental.pallas import tpu as pltpu
from jax.sharding import PartitionSpec as P

RMS_EPS = 1e-6
MESH = pl.DeviceIdType.MESH
BF16 = jnp.bfloat16
F32 = jnp.float32


def dot_nn(a, b):
    return lax.dot_general(a, b, (((1,), (0,)), ((), ())), preferred_element_type=F32)


def dot_nt(a, b):
    return lax.dot_general(a, b, (((1,), (1,)), ((), ())), preferred_element_type=F32)


def dot_tn(a, b):
    return lax.dot_general(a, b, (((0,), (0,)), ((), ())), preferred_element_type=F32)


def inv_rms(x):
    return lax.rsqrt(jnp.mean(x * x, axis=-1, keepdims=True) + RMS_EPS)


def rms_back(x, g):
    r = inv_rms(x)
    return r * g - x * (r * r * r) * jnp.mean(g * x, axis=-1, keepdims=True)


def activation(a, e):
    c0, c1 = 0.7978845608028654, 0.044715
    t = jnp.tanh(c0 * (a + c1 * (a * a * a)))
    half = 0.5 * (1.0 + t)
    slope = half + (0.5 * a) * ((1.0 + t) * (1.0 - t)) * (c0 * (1.0 + (3.0 * c1) * (a * a)))
    return (a * half).astype(BF16), (slope * e).astype(BF16)


class Ring:
    def __init__(self, place, buf, pieces, sems):
        self.place, self.buf, self.pieces = place, buf, pieces
        self.send_l, self.recv_l, self.send_s, self.recv_s, self.send_m, self.recv_m = sems

    def at(self, dev, p):
        j, row, rows = self.pieces[p]
        return self.buf.at[dev, j, pl.ds(row, rows)]

    def copy(self, dev, p, send, recv, to, src=None):
        ref = self.at(dev, p)
        return pltpu.make_async_remote_copy(
            src_ref=ref if src is None else src, dst_ref=ref, send_sem=send, recv_sem=recv,
            device_id={"tp": to}, device_id_type=MESH)

    def long(self, p, k):
        pc = self.place
        return self.copy(pc.slot(-k, 0), p, self.send_l.at[p, k], self.recv_l.at[p, k], pc.long_dev)

    def short(self, p, k):
        pc = self.place
        return self.copy(pc.slot(k, 0), p, self.send_s.at[p, k], self.recv_s.at[p, k], pc.short_dev)

    def start_own(self, p):
        pc = self.place
        self.long(p, 0).start()
        self.short(p, 0).start()
        self.copy(pc.me, p, self.send_m.at[p, 0], self.recv_m.at[p, 0], pc.mate).start()

    def step_long(self, p, k, forward=True):
        pc = self.place
        dev = pc.slot(-k, 0)
        self.copy(dev, p, self.send_l.at[p, k - 1], self.recv_l.at[p, k - 1], pc.long_dev).wait_recv()
        if forward:
            self.long(p, k).start()
        self.copy(dev, p, self.send_m.at[p, k], self.recv_m.at[p, k], pc.mate).start()

    def step_short(self, p, k, forward=True):
        pc = self.place
        dev = pc.slot(k, 0)
        far = pc.far
        self.copy(dev, p, self.send_s.at[p, k - 1], self.recv_s.at[p, k - 1], pc.short_dev).wait_recv()
        if forward is True:
            self.short(p, k).start()
        elif forward is not False:
            @pl.when(forward)
            def _():
                self.short(p, k).start()
        self.copy(dev, p, self.send_m.at[p, far + k], self.recv_m.at[p, far + k], pc.mate).start()

    def mate_own(self, p):
        pc = self.place
        self.copy(pc.mate, p, self.send_m.at[p, 0], self.recv_m.at[p, 0], pc.mate).wait_recv()

    def mate_long(self, p, k):
        pc = self.place
        self.copy(pc.slot(k, 1), p, self.send_m.at[p, k], self.recv_m.at[p, k], pc.mate).wait_recv()

    def mate_short(self, p, k):
        pc = self.place
        self.copy(pc.slot(-k, 1), p, self.send_m.at[p, pc.far + k], self.recv_m.at[p, pc.far + k], pc.mate).wait_recv()

    def drain(self):
        pc = self.place
        for p in range(len(self.pieces)):
            for k in range(pc.far):
                self.long(p, k).wait_send()
            for k in range(pc.far - 1):
                self.short(p, k).wait_send()
            for k in range(2 * pc.far):
                self.copy(pc.me, p, self.send_m.at[p, k], self.recv_m.at[p, k], pc.mate).wait_send()


class Place:
    def __init__(self, n_dev):
        self.n_dev, self.n_chip = n_dev, n_dev // 2
        self.far = self.n_chip // 2
        self.me = lax.axis_index("tp")
        self.chip, self.core = self.me // 2, lax.rem(self.me, 2)
        self.sign = 1 - 2 * self.core
        self.mate = 2 * self.chip + 1 - self.core
        self.long_dev = self.slot(1, 0)
        self.short_dev = self.slot(-1, 0)

    def slot(self, hops, other):
        chip = lax.rem(self.chip + hops * self.sign + self.n_chip, self.n_chip)
        return 2 * chip + (1 - self.core if other else self.core)


def kernel(n_dev, seqs, own, dim, scale,
           y1, y2, dy1, dy2, w1, w2, wo, wq,
           x1, x2, dyo, dx2, gq, go, gw1, gw2,
           xa, xb, w4, stage, packed, uc, w1t, w1raw, acc0, acc1, accw,
           a_sems, b_sems, c_sems, d_sems, load_sem, all_send, all_recv, free_sem):
    pc = Place(n_dev)
    me = pc.me
    toks = seqs * own
    hidden = y1.shape[1]
    group = seqs // 4
    far = pc.far

    loads = [(y1, x1), (dy2, dx2), (y2, x2), (dy1, dyo), (w2, xa.at[me, 1]), (w1, w1raw),
             (wo, w4.at[me, 0, pl.ds(0, dim)]), (wq.at[0], w4.at[me, 0, pl.ds(dim, dim)]),
             (wq.at[2], w4.at[me, 0, pl.ds(2 * dim, dim)]), (wq.at[1], w4.at[me, 0, pl.ds(3 * dim, dim)])]
    loads = [pltpu.make_async_copy(src, dst, load_sem.at[i]) for i, (src, dst) in enumerate(loads)]
    for i in (4, 5, 0, 1, 2, 3, 6, 7, 8, 9):
        loads[i].start()

    barrier = pltpu.get_barrier_semaphore()
    for hop in range(1, n_dev):
        pl.semaphore_signal(barrier, inc=1, device_id={"tp": lax.rem(me + hop, n_dev)}, device_id_type=MESH)
    pl.semaphore_wait(barrier, n_dev - 1)

    half = toks // 2
    ring_a = Ring(pc, xa, [(1, 0, toks), (0, 0, toks)], a_sems)
    ring_b = Ring(pc, xb, [(0, 0, half), (1, 0, half), (0, half, half), (1, half, half)], b_sems)
    ring_d = Ring(pc, w4, [(0, 0, 4 * dim)], d_sems)
    ring_c = Ring(pc, xa, [(0, 0, toks), (1, 0, toks)], c_sems)

    loads[4].wait()
    ring_a.start_own(0)
    loads[5].wait()
    turned = w1raw[...].T
    w1t[...] = turned
    xa[me, 0] = turned
    loads[0].wait()
    loads[1].wait()

    def norm_rows(i, _):
        rows = pl.ds(pl.multiple_of(i * 64, 64), 64)
        t = x1[rows]
        uc[0, rows] = (t * inv_rms(t)).astype(BF16)
        uc[1, rows] = dx2[rows].astype(BF16)
        return 0

    ring_a.start_own(1)
    lax.fori_loop(0, toks // 64, norm_rows, 0)
    acc0[...] = jnp.zeros_like(acc0)
    acc1[...] = jnp.zeros_like(acc1)
    for i in (2, 3, 6, 7, 8, 9):
        loads[i].wait()

    def mlp_rows(d):
        left, right = xa[d, 0], xa[d, 1]
        h, da = activation(dot_nt(uc[0], left), dot_nt(uc[1], right))
        acc0[...] += dot_nn(h, right)
        acc1[...] += dot_nn(da, left)

    def pair(chip_hops, body):
        chip = lax.rem(pc.chip + chip_hops + pc.n_chip, pc.n_chip)
        lax.fori_loop(0, 2, lambda i, _: (body(2 * chip + i), 0)[1], 0)

    def four(k, body):
        def one(i, _):
            chip = lax.rem(pc.chip + k * (1 - 2 * (i // 2)) + pc.n_chip, pc.n_chip)
            body(2 * chip + lax.rem(i, 2))
            return 0
        lax.fori_loop(0, 4, one, 0)

    def mates(ring, k, last):
        for p in range(len(ring.pieces)):
            ring.mate_long(p, k)
            if not last:
                ring.mate_short(p, k)

    def arrive(ring, k, last):
        for p in range(len(ring.pieces)):
            ring.step_long(p, k, forward=not last)
            if not last:
                ring.step_short(p, k, forward=k < far - 1)

    def ring_steps(rings, body, before_last):
        def step(k, _):
            for ring in rings:
                arrive(ring, k, False)
            for ring in rings:
                mates(ring, k, False)
            four(k, body)
            return 0
        lax.fori_loop(1, far, step, 0)
        before_last()
        for ring in rings:
            arrive(ring, far, True)
        for ring in rings:
            mates(ring, far, True)
        pair(far, body)

    for p in range(2):
        ring_a.mate_own(p)
    pair(0, mlp_rows)
    ring_steps([ring_a], mlp_rows, lambda: ring_d.start_own(0))

    def finish_mlp(i, _):
        rows = pl.ds(pl.multiple_of(i * 64, 64), 64)
        t = x2[rows] - acc0[rows]
        x2[rows] = t
        xb[me, 0, rows] = (t * inv_rms(t)).astype(BF16)
        g = dyo[rows] + rms_back(x1[rows], acc1[rows])
        dyo[rows] = g
        xb[me, 1, rows] = g.astype(BF16)
        return 0

    lax.fori_loop(0, half // 64, finish_mlp, 0)
    ring_b.start_own(0)
    ring_b.start_own(1)
    lax.fori_loop(half // 64, toks // 64, finish_mlp, 0)
    ring_b.start_own(2)
    ring_b.start_own(3)

    ring_a.drain()
    xa[me, 0] = uc[0]
    xa[me, 1] = uc[1]
    for dev in (pc.long_dev, pc.short_dev, pc.mate):
        pl.semaphore_signal(free_sem, inc=1, device_id={"tp": dev}, device_id_type=MESH)

    lane = lax.broadcasted_iota(jnp.int32, (toks, 4 * dim), 1)

    def project(d):
        w = w4[me, 0]
        stage[d] = jnp.where(lane < dim, dot_nt(xb[d, 1], w), dot_nt(xb[d, 0], w)).astype(BF16)

    for p in range(4):
        ring_b.mate_own(p)
    ring_d.mate_own(0)
    pair(0, project)

    def send_uc():
        pl.semaphore_wait(free_sem, 3)
        ring_c.start_own(0)
        ring_c.start_own(1)

    ring_steps([ring_d, ring_b], project, send_uc)

    go[...] = jnp.zeros_like(go)
    gq[...] = jnp.zeros_like(gq)
    low = lax.broadcasted_iota(jnp.int32, (n_dev * own, 2 * dim), 1) < dim
    none = jnp.zeros((n_dev * own, 2 * dim), BF16)

    def attend(s):
        rows = pl.ds(pl.multiple_of(s * own, own), own)
        block = stage[:, rows].reshape(n_dev * own, 4 * dim)
        left, right = block[:, :2 * dim], block[:, 2 * dim:]
        scores = dot_nt(jnp.where(low, none, left), right) * scale
        ex = jnp.exp(scores - jnp.max(scores, axis=-1, keepdims=True))
        prob = ex / jnp.sum(ex, axis=-1, keepdims=True)
        prob_b = prob.astype(BF16)
        d_prob = dot_nt(jnp.where(low, left, none), right)
        d_s = (prob * (d_prob - jnp.sum(d_prob * prob, axis=-1, keepdims=True)) * scale).astype(BF16)
        out_l = jnp.where(low, dot_nn(prob_b, right), dot_nn(d_s, right))
        out_r = jnp.where(low, dot_tn(prob_b, left), dot_tn(d_s, left))
        out = jnp.concatenate([out_l, out_r], axis=1).astype(BF16)
        stage[:, rows] = out.reshape(n_dev, own, 4 * dim)
        turn = out.T
        xs = xb[:, 0, rows].reshape(n_dev * own, hidden)
        cs = xb[:, 1, rows].reshape(n_dev * own, hidden)
        go[...] += dot_nn(turn[:dim], cs)
        g3 = dot_nn(turn[dim:], xs)
        gq[0] += g3[:dim]
        gq[2] += g3[dim:2 * dim]
        gq[1] += g3[2 * dim:]

    def back(g, hop):
        dev = lax.rem(me + hop, n_dev)
        rows = pl.ds(g * group * own, group * own)
        return pltpu.make_async_remote_copy(
            src_ref=stage.at[dev, rows], dst_ref=packed.at[me, rows],
            send_sem=all_send.at[g, hop - 1], recv_sem=all_recv.at[g, hop - 1],
            device_id={"tp": dev}, device_id_type=MESH)

    for g in range(4):
        lax.fori_loop(g * group, (g + 1) * group, lambda s, _: (attend(s), 0)[1], 0)
        for hop in range(1, n_dev):
            back(g, hop).start()

    gw2[...] = jnp.zeros_like(gw2)
    accw[...] = jnp.zeros_like(accw)
    w2v = pltpu.make_async_copy(w2, uc.at[0], load_sem.at[4])
    w2v.start()
    w2v.wait()

    def mlp_cols(d):
        ud, cd = xa[d, 0], xa[d, 1]
        h, da = activation(dot_nt(ud, w1t[...]), dot_nt(cd, uc[0]))
        gw2[...] += dot_tn(h, cd)
        accw[...] += dot_tn(da, ud)

    for p in range(2):
        ring_c.mate_own(p)
    pair(0, mlp_cols)

    def finish():
        packed[me] = stage[me]
        acc0[...] = jnp.zeros_like(acc0)
        acc1[...] = jnp.zeros_like(acc1)
        for hop in range(1, n_dev):
            src = lax.rem(me + n_dev - hop, n_dev)
            for g in range(4):
                rows = pl.ds(g * group * own, group * own)
                pltpu.make_async_remote_copy(
                    src_ref=stage.at[src, rows], dst_ref=packed.at[src, rows],
                    send_sem=all_send.at[g, hop - 1], recv_sem=all_recv.at[g, hop - 1],
                    device_id={"tp": src}, device_id_type=MESH).wait_recv()

        def head(n, _):
            pk = packed[n]
            w = w4[n, 0]
            zero = jnp.zeros_like(pk)
            acc0[...] += dot_nn(jnp.where(lane < dim, pk, zero), w)
            acc1[...] += dot_nn(jnp.where(lane < dim, zero, pk), w)
            return 0

        lax.fori_loop(0, n_dev, head, 0)

        def rows_out(i, _):
            rows = pl.ds(pl.multiple_of(i * 64, 64), 64)
            x1[rows] = x1[rows] - acc0[rows]
            dx2[rows] = dx2[rows] + rms_back(x2[rows], acc1[rows])
            return 0

        lax.fori_loop(0, toks // 64, rows_out, 0)

    ring_steps([ring_c], mlp_cols, finish)
    gw1[...] = accw[...].T
    ring_b.drain()
    ring_c.drain()
    ring_d.drain()
    for g in range(4):
        for hop in range(1, n_dev):
            back(g, hop).wait_send()


def layer_backward(n_dev, y_one, y_two, dy_one, dy_two, wq, wo, wu, wd):
    seqs, own, hidden = y_one.shape
    n_loc, dim = wo.shape[0], wo.shape[1]
    toks = seqs * own
    cols = wu.shape[1]
    flat = lambda t: t.reshape(toks, hidden)
    any_spec = pl.BlockSpec(memory_space=pl.ANY)
    vmem = pl.BlockSpec(memory_space=pltpu.VMEM)
    far = n_dev // 4

    def ring_sems(p):
        dma = pltpu.SemaphoreType.DMA
        return (dma((p, far)), dma((p, far)), dma((p, far - 1)), dma((p, far - 1)), dma((p, 2 * far)), dma((p, 2 * far)))

    body = functools.partial(kernel, n_dev, seqs, own, dim, dim ** -0.5)

    def flat_body(*refs):
        main, sems = refs[:16 + 11], refs[16 + 11:]
        rings = [sems[6 * i:6 * i + 6] for i in range(4)]
        body(*main, *rings, *sems[24:])

    sems = [s for p in (2, 4, 2, 1) for s in ring_sems(p)]
    dma = pltpu.SemaphoreType.DMA
    outs = pl.pallas_call(
        flat_body,
        name="reversible_block",
        out_shape=[jax.ShapeDtypeStruct((toks, hidden), F32)] * 4 + [
            jax.ShapeDtypeStruct((3, dim, hidden), F32), jax.ShapeDtypeStruct((dim, hidden), F32),
            jax.ShapeDtypeStruct((hidden, cols), F32), jax.ShapeDtypeStruct((cols, hidden), F32)],
        in_specs=[any_spec] * 8,
        out_specs=[vmem] * 8,
        scratch_shapes=[
            pltpu.VMEM((n_dev, 2, toks, hidden), BF16),
            pltpu.VMEM((n_dev, 2, toks, hidden), BF16),
            pltpu.VMEM((n_dev, 1, 4 * dim, hidden), BF16),
            pltpu.VMEM((n_dev, toks, 4 * dim), BF16),
            pltpu.VMEM((n_dev, toks, 4 * dim), BF16),
            pltpu.VMEM((2, toks, hidden), BF16),
            pltpu.VMEM((cols, hidden), BF16),
            pltpu.VMEM((hidden, cols), BF16),
            pltpu.VMEM((toks, hidden), F32),
            pltpu.VMEM((toks, hidden), F32),
            pltpu.VMEM((cols, hidden), F32),
            *sems,
            dma((10,)),
            dma((4, n_dev - 1)),
            dma((4, n_dev - 1)),
            pltpu.SemaphoreType.REGULAR,
        ],
        compiler_params=pltpu.CompilerParams(collective_id=0, has_side_effects=True, vmem_limit_bytes=67043328),
    )(flat(y_one), flat(y_two), flat(dy_one), flat(dy_two), wu, wd, wo.reshape(n_loc * dim, hidden), wq.transpose(1, 2, 3, 0).reshape(3, dim, hidden))
    x_one, x_two, dx_one, dx_two, g_q, g_o, g_up, g_down = outs
    back = lambda t: t.reshape(y_one.shape)
    return back(x_one), back(x_two), back(dx_one), back(dx_two), g_q.reshape(n_loc, 3, dim, hidden).transpose(3, 0, 1, 2), g_o.reshape(wo.shape), g_up, g_down


def local_backward(n_dev, y_one, y_two, dy_one, dy_two, w_qkv, w_out, w_up, w_down):
    grads = []
    state = (y_one, y_two, dy_one, dy_two)
    for idx in reversed(range(w_qkv.shape[0])):
        res = layer_backward(n_dev, *state, w_qkv[idx], w_out[idx], w_up[idx], w_down[idx])
        state = res[:4]
        grads.append(res[4:])
    return state + tuple(jnp.stack(g[::-1]) for g in zip(*grads))


def solution(mesh):
    state_spec = P("dp", "tp", None)
    in_specs = (state_spec, state_spec, state_spec, state_spec, P(None, None, "tp", None, None), P(None, "tp", None, None), P(None, None, "tp"), P(None, "tp", None))
    out_specs = (state_spec, state_spec, state_spec, state_spec, P("dp", None, "tp", None, None), P("dp", "tp", None, None), P("dp", None, "tp"), P("dp", "tp", None))
    return jax.shard_map(functools.partial(local_backward, mesh.shape["tp"]), mesh=mesh, in_specs=in_specs, out_specs=out_specs, check_vma=False)
```

```python
import functools

import jax
import jax.numpy as jnp
from jax import lax
from jax.experimental import pallas as pl
from jax.experimental.pallas import tpu as pltpu
from jax.sharding import PartitionSpec as P

RMS_EPS = 1e-6
VMEM_GRANT = 56 * 1024 * 1024
MESH = pl.DeviceIdType.MESH
BF16 = jnp.bfloat16
F32 = jnp.float32


def dot_nn(a, b):
    return lax.dot_general(a, b, (((1,), (0,)), ((), ())), preferred_element_type=F32)


def dot_nt(a, b):
    return lax.dot_general(a, b, (((1,), (1,)), ((), ())), preferred_element_type=F32)


def dot_tn(a, b):
    return lax.dot_general(a, b, (((0,), (0,)), ((), ())), preferred_element_type=F32)


def inv_rms(x):
    return lax.rsqrt(jnp.mean(x * x, axis=-1, keepdims=True) + RMS_EPS)


def rms_back(x, g):
    r = inv_rms(x)
    return r * g - x * (r * r * r) * jnp.mean(g * x, axis=-1, keepdims=True)


def activation(a, e):
    c0, c1 = 0.7978845608028654, 0.044715
    t = jnp.tanh(c0 * (a + c1 * (a * a * a)))
    half = 0.5 * (1.0 + t)
    slope = half + (0.5 * a) * ((1.0 + t) * (1.0 - t)) * (c0 * (1.0 + (3.0 * c1) * (a * a)))
    return (a * half).astype(BF16), (slope * e).astype(BF16)


class Ring:
    def __init__(self, place, buf, pieces, sems):
        self.place, self.buf, self.pieces = place, buf, pieces
        self.send_l, self.recv_l, self.send_s, self.recv_s, self.send_m, self.recv_m = sems

    def at(self, dev, p):
        j, row, rows = self.pieces[p]
        return self.buf.at[dev, j, pl.ds(row, rows)]

    def copy(self, dev, p, send, recv, to, src=None):
        ref = self.at(dev, p)
        return pltpu.make_async_remote_copy(
            src_ref=ref if src is None else src, dst_ref=ref, send_sem=send, recv_sem=recv,
            device_id={"tp": to}, device_id_type=MESH)

    def long(self, p, k):
        pc = self.place
        return self.copy(pc.slot(-k, 0), p, self.send_l.at[p, k], self.recv_l.at[p, k], pc.long_dev)

    def short(self, p, k):
        pc = self.place
        return self.copy(pc.slot(k, 0), p, self.send_s.at[p, k], self.recv_s.at[p, k], pc.short_dev)

    def start_own(self, p):
        pc = self.place
        self.long(p, 0).start()
        self.short(p, 0).start()
        self.copy(pc.me, p, self.send_m.at[p, 0], self.recv_m.at[p, 0], pc.mate).start()

    def step_long(self, p, k, forward=True):
        pc = self.place
        dev = pc.slot(-k, 0)
        self.copy(dev, p, self.send_l.at[p, k - 1], self.recv_l.at[p, k - 1], pc.long_dev).wait_recv()
        if forward:
            self.long(p, k).start()
        self.copy(dev, p, self.send_m.at[p, k], self.recv_m.at[p, k], pc.mate).start()

    def step_short(self, p, k, forward=True):
        pc = self.place
        dev = pc.slot(k, 0)
        far = pc.far
        self.copy(dev, p, self.send_s.at[p, k - 1], self.recv_s.at[p, k - 1], pc.short_dev).wait_recv()
        if forward is True:
            self.short(p, k).start()
        elif forward is not False:
            @pl.when(forward)
            def _():
                self.short(p, k).start()
        self.copy(dev, p, self.send_m.at[p, far + k], self.recv_m.at[p, far + k], pc.mate).start()

    def mate_own(self, p):
        pc = self.place
        self.copy(pc.mate, p, self.send_m.at[p, 0], self.recv_m.at[p, 0], pc.mate).wait_recv()

    def mate_long(self, p, k):
        pc = self.place
        self.copy(pc.slot(k, 1), p, self.send_m.at[p, k], self.recv_m.at[p, k], pc.mate).wait_recv()

    def mate_short(self, p, k):
        pc = self.place
        self.copy(pc.slot(-k, 1), p, self.send_m.at[p, pc.far + k], self.recv_m.at[p, pc.far + k], pc.mate).wait_recv()

    def drain(self):
        pc = self.place
        for p in range(len(self.pieces)):
            for k in range(pc.far):
                self.long(p, k).wait_send()
            for k in range(pc.far - 1):
                self.short(p, k).wait_send()
            for k in range(2 * pc.far):
                self.copy(pc.me, p, self.send_m.at[p, k], self.recv_m.at[p, k], pc.mate).wait_send()


class Place:
    def __init__(self, n_dev):
        self.n_dev, self.n_chip = n_dev, n_dev // 2
        self.far = self.n_chip // 2
        self.me = lax.axis_index("tp")
        self.chip, self.core = self.me // 2, lax.rem(self.me, 2)
        self.sign = 1 - 2 * self.core
        self.mate = 2 * self.chip + 1 - self.core
        self.long_dev = self.slot(1, 0)
        self.short_dev = self.slot(-1, 0)

    def slot(self, hops, other):
        chip = lax.rem(self.chip + hops * self.sign + self.n_chip, self.n_chip)
        return 2 * chip + (1 - self.core if other else self.core)


def kernel(n_dev, seqs, own, dim, scale,
           y1, y2, dy1, dy2, w1, w2, wo, wq,
           x1, x2, dyo, dx2, gq, go, gw1, gw2,
           xa, xb, w4, stage, uc, w1t, w2own, w1raw, acc0, acc1, accw, o_out, o_in, du_in,
           a_sems, b_sems, c_sems, d_sems, load_sem, all_send, all_recv, free_sem):
    pc = Place(n_dev)
    me = pc.me
    toks = seqs * own
    hidden = y1.shape[1]
    group = seqs // 4
    far = pc.far

    loads = [(y1, x1), (dy2, dx2), (y2, x2), (dy1, dyo), (w2, xa.at[me, 1]), (w1, w1raw),
             (wo, w4.at[me, 0, pl.ds(0, dim)]), (wq.at[0], w4.at[me, 0, pl.ds(dim, dim)]),
             (wq.at[2], w4.at[me, 0, pl.ds(2 * dim, dim)]), (wq.at[1], w4.at[me, 0, pl.ds(3 * dim, dim)]), (w2, w2own)]
    loads = [pltpu.make_async_copy(src, dst, load_sem.at[i]) for i, (src, dst) in enumerate(loads)]
    for i in (4, 5, 0, 1, 2, 3, 6, 7, 8, 9, 10):
        loads[i].start()

    with jax.named_scope("barrier"):
        barrier = pltpu.get_barrier_semaphore()
        for dev in (pc.long_dev, pc.short_dev, pc.mate):
            pl.semaphore_signal(barrier, inc=1, device_id={"tp": dev}, device_id_type=MESH)
        pl.semaphore_wait(barrier, 3)

    half = toks // 2
    ring_a = Ring(pc, xa, [(1, 0, toks), (0, 0, toks)], a_sems)
    ring_b = Ring(pc, xb, [(0, 0, half), (1, 0, half), (0, half, half), (1, half, half)], b_sems)
    ring_d = Ring(pc, w4, [(0, 0, 4 * dim)], d_sems)
    ring_c = Ring(pc, xa, [(0, 0, half), (1, 0, half), (0, half, half), (1, half, half)], c_sems)

    loads[4].wait()
    ring_a.start_own(0)
    loads[5].wait()
    turned = w1raw[...].T
    w1t[...] = turned
    xa[me, 0] = turned
    loads[0].wait()
    loads[1].wait()

    def norm_rows(i, _):
        rows = pl.ds(pl.multiple_of(i * 64, 64), 64)
        t = x1[rows]
        uc[0, rows] = (t * inv_rms(t)).astype(BF16)
        uc[1, rows] = dx2[rows].astype(BF16)
        return 0

    ring_a.start_own(1)
    lax.fori_loop(0, toks // 64, norm_rows, 0)
    acc0[...] = jnp.zeros_like(acc0)
    acc1[...] = jnp.zeros_like(acc1)
    for i in (2, 3, 6, 7, 8, 9, 10):
        loads[i].wait()

    def mlp_rows(d):
        left, right = xa[d, 0], xa[d, 1]
        h, da = activation(dot_nt(uc[0], left), dot_nt(uc[1], right))
        acc0[...] += dot_nn(h, right)
        acc1[...] += dot_nn(da, left)

    def pair(chip_hops, body):
        chip = lax.rem(pc.chip + chip_hops + pc.n_chip, pc.n_chip)
        lax.fori_loop(0, 2, lambda i, _: (body(2 * chip + i), 0)[1], 0)

    def four(k, body):
        def one(i, _):
            chip = lax.rem(pc.chip + k * (1 - 2 * (i // 2)) + pc.n_chip, pc.n_chip)
            body(2 * chip + lax.rem(i, 2))
            return 0
        lax.fori_loop(0, 4, one, 0)

    def mates(ring, k, last, pieces=None):
        for p in pieces or range(len(ring.pieces)):
            ring.mate_long(p, k)
            if not last:
                ring.mate_short(p, k)

    def arrive(ring, k, last, pieces=None):
        for p in pieces or range(len(ring.pieces)):
            ring.step_long(p, k, forward=not last)
            if not last:
                ring.step_short(p, k, forward=k < far - 1)

    def ring_steps(rings, body, before_last):
        def step(k, _):
            with jax.named_scope("arrive"):
                for ring in rings:
                    arrive(ring, k, False)
            with jax.named_scope("mates"):
                for ring in rings:
                    mates(ring, k, False)
            with jax.named_scope("compute"):
                four(k, body)
            return 0
        lax.fori_loop(1, far, step, 0)
        with jax.named_scope("before_last"):
            before_last()
        with jax.named_scope("arrive_last"):
            for ring in rings:
                arrive(ring, far, True)
        with jax.named_scope("mates_last"):
            for ring in rings:
                mates(ring, far, True)
        with jax.named_scope("compute_last"):
            pair(far, body)

    for p in range(2):
        ring_a.mate_own(p)
    pair(0, mlp_rows)
    ring_steps([ring_a], mlp_rows, lambda: ring_d.start_own(0))

    def finish_mlp(i, _):
        rows = pl.ds(pl.multiple_of(i * 64, 64), 64)
        t = x2[rows] - acc0[rows]
        x2[rows] = t
        xb[me, 0, rows] = (t * inv_rms(t)).astype(BF16)
        g = dyo[rows] + rms_back(x1[rows], acc1[rows])
        dyo[rows] = g
        xb[me, 1, rows] = g.astype(BF16)
        return 0

    with jax.named_scope("finish_mlp"):
        lax.fori_loop(0, half // 64, finish_mlp, 0)
    ring_b.start_own(0)
    ring_b.start_own(1)
    lax.fori_loop(half // 64, toks // 64, finish_mlp, 0)
    ring_b.start_own(2)
    ring_b.start_own(3)

    with jax.named_scope("drain_a"):
        ring_a.drain()
    xa[me, 0] = uc[0]
    xa[me, 1] = uc[1]
    for dev in (pc.long_dev, pc.short_dev, pc.mate):
        pl.semaphore_signal(free_sem, inc=1, device_id={"tp": dev}, device_id_type=MESH)

    lane = lax.broadcasted_iota(jnp.int32, (toks, 4 * dim), 1)

    def project(d):
        w = w4[me, 0]
        stage[d] = jnp.where(lane < dim, dot_nt(xb[d, 1], w), dot_nt(xb[d, 0], w)).astype(BF16)

    for p in range(4):
        ring_b.mate_own(p)
    ring_d.mate_own(0)
    pair(0, project)

    def send_uc():
        pl.semaphore_wait(free_sem, 3)
        for p in range(4):
            ring_c.start_own(p)

    ring_steps([ring_d, ring_b], project, send_uc)

    full = n_dev * own
    low = lax.broadcasted_iota(jnp.int32, (full, 2 * dim), 1) < dim
    none = jnp.zeros((full, 2 * dim), BF16)

    def attend(block):
        left, right = block[:, :2 * dim], block[:, 2 * dim:]
        scores = dot_nt(jnp.where(low, none, left), right) * scale
        ex = jnp.exp(scores - jnp.max(scores, axis=-1, keepdims=True))
        prob = ex / jnp.sum(ex, axis=-1, keepdims=True)
        prob_b = prob.astype(BF16)
        d_prob = dot_nt(jnp.where(low, left, none), right)
        d_s = (prob * (d_prob - jnp.sum(d_prob * prob, axis=-1, keepdims=True)) * scale).astype(BF16)
        out_l = jnp.where(low, dot_nn(prob_b, right), dot_nn(d_s, right))
        out_r = jnp.where(low, dot_tn(prob_b, left), dot_tn(d_s, left))
        return out_l, out_r

    mine = pl.ds(pl.multiple_of(me * own, own), own)
    uc[0] = xb[:, 0, mine].reshape(full, hidden)
    uc[1] = xb[:, 1, mine].reshape(full, hidden)
    acc0[...] = jnp.zeros_like(acc0)

    def two_heads(i, _):
        o_pair, du = [], None
        for j in range(2):
            w = w4[2 * i + j, 0]
            block = jnp.where(lane < dim, dot_nt(uc[1], w), dot_nt(uc[0], w)).astype(BF16)
            out_l, out_r = attend(block)
            o_pair.append(out_l)
            out = jnp.concatenate([out_l, out_r], axis=1)
            part = dot_nn(jnp.where(lane < dim, 0.0, out).astype(BF16), w)
            du = part if du is None else du + part
        acc0[...] += du
        o_out[:, pl.ds(pl.multiple_of(i * 2 * dim, 2 * dim), 2 * dim)] = jnp.where(
            low, o_pair[0], pltpu.roll(o_pair[1], dim, axis=1)).astype(BF16)
        return 0

    n_pair = n_dev // 2
    with jax.named_scope("own_seq"):
        lax.fori_loop(0, n_pair // 2, two_heads, 0)
    with jax.named_scope("arrive_c1"):
        arrive(ring_c, 1, False)
    with jax.named_scope("own_seq"):
        lax.fori_loop(n_pair // 2, n_pair, two_heads, 0)

    def back(src_buf, dst_buf, i, hop):
        dev = lax.rem(me + hop, n_dev)
        theirs = pl.ds(pl.multiple_of(dev * own, own), own)
        return pltpu.make_async_remote_copy(
            src_ref=src_buf.at[theirs], dst_ref=dst_buf.at[mine],
            send_sem=all_send.at[i, hop - 1], recv_sem=all_recv.at[i, hop - 1],
            device_id={"tp": dev}, device_id_type=MESH)

    backs = [(o_out, o_in, 0), (acc0, du_in, 1)]
    for hop in range(1, n_dev):
        for args in backs:
            back(*args, hop).start()

    go[...] = jnp.zeros_like(go)
    gq[...] = jnp.zeros_like(gq)

    def own_head(s, _):
        rows = pl.ds(pl.multiple_of(s * own, own), own)
        out_l, out_r = attend(stage[:, rows].reshape(full, 4 * dim))
        turn = jnp.concatenate([out_l, out_r], axis=1).astype(BF16).T
        go[...] += dot_nn(turn[:dim], xb[:, 1, rows].reshape(full, hidden))
        g3 = dot_nn(turn[dim:], xb[:, 0, rows].reshape(full, hidden))
        gq[0] += g3[:dim]
        gq[2] += g3[dim:2 * dim]
        gq[1] += g3[2 * dim:]
        return 0

    gw2[...] = jnp.zeros_like(gw2)
    accw[...] = jnp.zeros_like(accw)

    def cols(ud, cd):
        h, da = activation(dot_nt(ud, w1t[...]), dot_nt(cd, w2own[...]))
        gw2[...] += dot_tn(h, cd)
        accw[...] += dot_tn(da, ud)

    def mlp_cols(d):
        cols(xa[d, 0], xa[d, 1])

    def finish():
        o_in[mine] = o_out[mine]
        du_in[mine] = acc0[mine]
        with jax.named_scope("wait_back"):
            for hop in range(1, n_dev):
                src = lax.rem(me + n_dev - hop, n_dev)
                theirs = pl.ds(pl.multiple_of(src * own, own), own)
                for buf, i in ((o_in, 0), (du_in, 1)):
                    pltpu.make_async_remote_copy(
                        src_ref=buf.at[theirs], dst_ref=buf.at[theirs],
                        send_sem=all_send.at[i, hop - 1], recv_sem=all_recv.at[i, hop - 1],
                        device_id={"tp": src}, device_id_type=MESH).wait_recv()
        x1[...] = x1[...] - dot_nn(o_in[...], w4[:, 0, pl.ds(0, dim)].reshape(n_dev * dim, hidden))

        def rows_out(i, _):
            rows = pl.ds(pl.multiple_of(i * 64, 64), 64)
            dx2[rows] = dx2[rows] + rms_back(x2[rows], du_in[rows])
            return 0

        lax.fori_loop(0, toks // 64, rows_out, 0)

    with jax.named_scope("own_cols"):
        for p in range(4):
            ring_c.mate_own(p)
        pair(0, mlp_cols)
    with jax.named_scope("cols_1"):
        mates(ring_c, 1, False)
        four(1, mlp_cols)
    with jax.named_scope("own_head"):
        lax.fori_loop(0, seqs // 2, own_head, 0)
    with jax.named_scope("arrive_c2"):
        arrive(ring_c, 2, False)
    with jax.named_scope("cols_2"):
        mates(ring_c, 2, False)
        four(2, mlp_cols)
    with jax.named_scope("own_head"):
        lax.fori_loop(seqs // 2, seqs, own_head, 0)
    for k in range(3, far):
        with jax.named_scope("arrive_c3"):
            arrive(ring_c, k, False)
        with jax.named_scope("cols_3"):
            mates(ring_c, k, False)
            four(k, mlp_cols)
    with jax.named_scope("finish"):
        finish()
    for part in range(2):
        pieces = (2 * part, 2 * part + 1)
        with jax.named_scope("arrive_c4"):
            arrive(ring_c, far, True, pieces)
        with jax.named_scope("mates_c4"):
            mates(ring_c, far, True, pieces)
        with jax.named_scope("cols_4"):
            rows = pl.ds(part * half, half)
            pair(far, lambda d: cols(xa[d, 0, rows], xa[d, 1, rows]))
    with jax.named_scope("tail"):
        gw1[...] = accw[...].T
        ring_b.drain()
        ring_c.drain()
        ring_d.drain()
        for hop in range(1, n_dev):
            for args in backs:
                back(*args, hop).wait_send()


def writer(*refs):
    n = len(refs) // 2
    copies = [pltpu.make_async_copy(refs[i], refs[n + i], refs[-1].at[i]) for i in range(n)]
    for copy in copies:
        copy.start()
    for copy in copies:
        copy.wait()


def layer_backward(n_dev, y_one, y_two, dy_one, dy_two, wq, wo, wu, wd):
    seqs, own, hidden = y_one.shape
    n_loc, dim = wo.shape[0], wo.shape[1]
    toks = seqs * own
    cols = wu.shape[1]
    flat = lambda t: t.reshape(toks, hidden)
    any_spec = pl.BlockSpec(memory_space=pl.ANY)
    vmem = pl.BlockSpec(memory_space=pltpu.VMEM)
    far = n_dev // 4

    def ring_sems(p):
        dma = pltpu.SemaphoreType.DMA
        return (dma((p, far)), dma((p, far)), dma((p, far - 1)), dma((p, far - 1)), dma((p, 2 * far)), dma((p, 2 * far)))

    body = functools.partial(kernel, n_dev, seqs, own, dim, dim ** -0.5)

    def flat_body(*refs):
        main, sems = refs[:16 + 14], refs[16 + 14:]
        rings = [sems[6 * i:6 * i + 6] for i in range(4)]
        body(*main, *rings, *sems[24:])

    sems = [s for p in (2, 4, 4, 1) for s in ring_sems(p)]
    dma = pltpu.SemaphoreType.DMA
    shapes = [(toks, hidden)] * 4 + [(3, dim, hidden), (dim, hidden), (hidden, cols), (cols, hidden)]
    outs = pl.pallas_call(
        flat_body,
        name="reversible_block",
        out_shape=[pltpu.VMEM(shape, F32) for shape in shapes],
        in_specs=[any_spec] * 8,
        out_specs=[vmem] * 8,
        scratch_shapes=[
            pltpu.VMEM((n_dev, 2, toks, hidden), BF16),
            pltpu.VMEM((n_dev, 2, toks, hidden), BF16),
            pltpu.VMEM((n_dev, 1, 4 * dim, hidden), BF16),
            pltpu.VMEM((n_dev, toks, 4 * dim), BF16),
            pltpu.VMEM((2, toks, hidden), BF16),
            pltpu.VMEM((cols, hidden), BF16),
            pltpu.VMEM((cols, hidden), BF16),
            pltpu.VMEM((hidden, cols), BF16),
            pltpu.VMEM((toks, hidden), F32),
            pltpu.VMEM((toks, hidden), F32),
            pltpu.VMEM((cols, hidden), F32),
            pltpu.VMEM((toks, hidden), BF16),
            pltpu.VMEM((toks, hidden), BF16),
            pltpu.VMEM((toks, hidden), F32),
            *sems,
            dma((11,)),
            dma((2, n_dev - 1)),
            dma((2, n_dev - 1)),
            pltpu.SemaphoreType.REGULAR,
        ],
        compiler_params=pltpu.CompilerParams(collective_id=0, has_side_effects=True, vmem_limit_bytes=VMEM_GRANT),
    )(flat(y_one), flat(y_two), flat(dy_one), flat(dy_two), wu, wd, wo.reshape(n_loc * dim, hidden), wq.transpose(1, 2, 3, 0).reshape(3, dim, hidden))
    outs = pl.pallas_call(
        writer,
        name="write_results",
        out_shape=[jax.ShapeDtypeStruct(shape, F32) for shape in shapes],
        in_specs=[vmem] * 8,
        out_specs=[any_spec] * 8,
        scratch_shapes=[dma((8,))],
        compiler_params=pltpu.CompilerParams(vmem_limit_bytes=1024 * 1024),
    )(*[pltpu.with_memory_space_constraint(t, pltpu.VMEM) for t in outs])
    x_one, x_two, dx_one, dx_two, g_q, g_o, g_up, g_down = outs
    back = lambda t: t.reshape(y_one.shape)
    return back(x_one), back(x_two), back(dx_one), back(dx_two), g_q.reshape(n_loc, 3, dim, hidden).transpose(3, 0, 1, 2), g_o.reshape(wo.shape), g_up, g_down


def local_backward(n_dev, y_one, y_two, dy_one, dy_two, w_qkv, w_out, w_up, w_down):
    grads = []
    state = (y_one, y_two, dy_one, dy_two)
    for idx in reversed(range(w_qkv.shape[0])):
        res = layer_backward(n_dev, *state, w_qkv[idx], w_out[idx], w_up[idx], w_down[idx])
        state = res[:4]
        grads.append(res[4:])
    return state + tuple(jnp.stack(g[::-1]) for g in zip(*grads))


def solution(mesh):
    state_spec = P("dp", "tp", None)
    in_specs = (state_spec, state_spec, state_spec, state_spec, P(None, None, "tp", None, None), P(None, "tp", None, None), P(None, None, "tp"), P(None, "tp", None))
    out_specs = (state_spec, state_spec, state_spec, state_spec, P("dp", None, "tp", None, None), P("dp", "tp", None, None), P("dp", None, "tp"), P("dp", "tp", None))
    return jax.shard_map(functools.partial(local_backward, mesh.shape["tp"]), mesh=mesh, in_specs=in_specs, out_specs=out_specs, check_vma=False)
```

```python
import functools

import jax
import jax.numpy as jnp
from jax import lax
from jax.experimental import pallas as pl
from jax.experimental.pallas import tpu as pltpu
from jax.sharding import PartitionSpec as P

RMS_EPS = 1e-6
VMEM_GRANT = 56 * 1024 * 1024
MESH = pl.DeviceIdType.MESH
BF16 = jnp.bfloat16
F32 = jnp.float32


def dot_nn(a, b):
    return lax.dot_general(a, b, (((1,), (0,)), ((), ())), preferred_element_type=F32)


def dot_nt(a, b):
    return lax.dot_general(a, b, (((1,), (1,)), ((), ())), preferred_element_type=F32)


def dot_tn(a, b):
    return lax.dot_general(a, b, (((0,), (0,)), ((), ())), preferred_element_type=F32)


def inv_rms(x):
    return lax.rsqrt(jnp.mean(x * x, axis=-1, keepdims=True) + RMS_EPS)


def rms_back(x, g):
    r = inv_rms(x)
    return r * g - x * (r * r * r) * jnp.mean(g * x, axis=-1, keepdims=True)


def activation(a, e):
    c0, c1 = 0.7978845608028654, 0.044715
    t = jnp.tanh(c0 * (a + c1 * (a * a * a)))
    half = 0.5 * (1.0 + t)
    slope = half + (0.5 * a) * ((1.0 + t) * (1.0 - t)) * (c0 * (1.0 + (3.0 * c1) * (a * a)))
    return (a * half).astype(BF16), (slope * e).astype(BF16)


class Ring:
    def __init__(self, place, buf, pieces, sems):
        self.place, self.buf, self.pieces = place, buf, pieces
        self.sent, self.recv_l, self.recv_s, self.recv_m = sems

    def at(self, dev, p):
        j, row, rows = self.pieces[p]
        return self.buf.at[dev, j, pl.ds(row, rows)]

    def copy(self, dev, p, recv, to):
        ref = self.at(dev, p)
        return pltpu.make_async_remote_copy(
            src_ref=ref, dst_ref=ref, send_sem=self.sent, recv_sem=recv, device_id={"tp": to}, device_id_type=MESH)

    def long(self, p, k):
        pc = self.place
        return self.copy(pc.slot(-k, 0), p, self.recv_l.at[p, k], pc.long_dev)

    def short(self, p, k):
        pc = self.place
        return self.copy(pc.slot(k, 0), p, self.recv_s.at[p, k], pc.short_dev)

    def start_own(self, p):
        pc = self.place
        self.long(p, 0).start()
        self.short(p, 0).start()
        self.copy(pc.me, p, self.recv_m.at[p, 0], pc.mate).start()

    def step_long(self, p, k, forward=True):
        pc = self.place
        dev = pc.slot(-k, 0)
        self.copy(dev, p, self.recv_l.at[p, k - 1], pc.long_dev).wait_recv()
        if forward:
            self.long(p, k).start()
        self.copy(dev, p, self.recv_m.at[p, k], pc.mate).start()

    def step_short(self, p, k, forward=True):
        pc = self.place
        dev = pc.slot(k, 0)
        far = pc.far
        self.copy(dev, p, self.recv_s.at[p, k - 1], pc.short_dev).wait_recv()
        if forward is True:
            self.short(p, k).start()
        elif forward is not False:
            @pl.when(forward)
            def _():
                self.short(p, k).start()
        self.copy(dev, p, self.recv_m.at[p, far + k], pc.mate).start()

    def mate_own(self, p):
        pc = self.place
        self.copy(pc.mate, p, self.recv_m.at[p, 0], pc.mate).wait_recv()

    def mate_long(self, p, k):
        pc = self.place
        self.copy(pc.slot(k, 1), p, self.recv_m.at[p, k], pc.mate).wait_recv()

    def mate_short(self, p, k):
        pc = self.place
        self.copy(pc.slot(-k, 1), p, self.recv_m.at[p, pc.far + k], pc.mate).wait_recv()

    def drain(self):
        all_sent = self.buf.at[pl.ds(0, self.place.n_dev - 1)]
        pltpu.make_async_copy(all_sent, all_sent, self.sent).wait()


class Place:
    def __init__(self, n_dev):
        self.n_dev, self.n_chip = n_dev, n_dev // 2
        self.far = self.n_chip // 2
        self.me = lax.axis_index("tp")
        self.chip, self.core = self.me // 2, lax.rem(self.me, 2)
        self.sign = 1 - 2 * self.core
        self.mate = 2 * self.chip + 1 - self.core
        self.long_dev = self.slot(1, 0)
        self.short_dev = self.slot(-1, 0)

    def slot(self, hops, other):
        chip = lax.rem(self.chip + hops * self.sign + self.n_chip, self.n_chip)
        return 2 * chip + (1 - self.core if other else self.core)


def kernel(n_dev, seqs, own, dim, scale,
           y1, y2, dy1, dy2, w1, w2, wo, wq,
           x1, x2, dyo, dx2, gq, go, accw, gw2,
           xa, xb, w4, stage, uc, w1t, w2own, w1raw, acc0, acc1, o_out, o_in, du_in,
           a_sems, b_sems, c_sems, d_sems, load_sem, all_send, all_recv, free_sem):
    pc = Place(n_dev)
    me = pc.me
    toks = seqs * own
    hidden = y1.shape[1]
    group = seqs // 4
    far = pc.far

    loads = [(y1, x1), (dy2, dx2), (y2, x2), (dy1, dyo), (w2, xa.at[me, 1]), (w1, w1raw),
             (wo, w4.at[me, 0, pl.ds(0, dim)]), (wq.at[0], w4.at[me, 0, pl.ds(dim, dim)]),
             (wq.at[2], w4.at[me, 0, pl.ds(2 * dim, dim)]), (wq.at[1], w4.at[me, 0, pl.ds(3 * dim, dim)]), (w2, w2own)]
    loads = [pltpu.make_async_copy(src, dst, load_sem.at[i]) for i, (src, dst) in enumerate(loads)]
    for i in (4, 5, 0, 1, 2, 3, 6, 7, 8, 9, 10):
        loads[i].start()

    with jax.named_scope("barrier"):
        barrier = pltpu.get_barrier_semaphore()
        for dev in (pc.long_dev, pc.short_dev, pc.mate):
            pl.semaphore_signal(barrier, inc=1, device_id={"tp": dev}, device_id_type=MESH)
        pl.semaphore_wait(barrier, 3)

    half = toks // 2
    ring_a = Ring(pc, xa, [(1, 0, toks), (0, 0, toks)], a_sems)
    ring_b = Ring(pc, xb, [(0, 0, toks), (1, 0, toks)], b_sems)
    ring_d = Ring(pc, w4, [(0, 0, 4 * dim)], d_sems)
    both = pl.ds(0, 2)
    ring_c = Ring(pc, xa, [(both, 0, half), (both, half, half)], c_sems)

    loads[4].wait()
    ring_a.start_own(0)
    loads[5].wait()
    turned = w1raw[...].T
    w1t[...] = turned
    xa[me, 0] = turned
    loads[0].wait()
    loads[1].wait()

    def norm_rows(i, _):
        rows = pl.ds(pl.multiple_of(i * 64, 64), 64)
        t = x1[rows]
        uc[0, rows] = (t * inv_rms(t)).astype(BF16)
        uc[1, rows] = dx2[rows].astype(BF16)
        return 0

    ring_a.start_own(1)
    lax.fori_loop(0, toks // 64, norm_rows, 0)
    acc0[...] = jnp.zeros_like(acc0)
    acc1[...] = jnp.zeros_like(acc1)
    for i in (2, 3, 6, 7, 8, 9, 10):
        loads[i].wait()

    def mlp_rows(d):
        left, right = xa[d, 0], xa[d, 1]
        h, da = activation(dot_nt(uc[0], left), dot_nt(uc[1], right))
        acc0[...] += dot_nn(h, right)
        acc1[...] += dot_nn(da, left)

    def pair(chip_hops, body):
        chip = lax.rem(pc.chip + chip_hops + pc.n_chip, pc.n_chip)
        lax.fori_loop(0, 2, lambda i, _: (body(2 * chip + i), 0)[1], 0)

    def four(k, body):
        def one(i, _):
            chip = lax.rem(pc.chip + k * (1 - 2 * (i // 2)) + pc.n_chip, pc.n_chip)
            body(2 * chip + lax.rem(i, 2))
            return 0
        lax.fori_loop(0, 4, one, 0)

    def mates(ring, k, last, pieces=None):
        for p in pieces or range(len(ring.pieces)):
            ring.mate_long(p, k)
            if not last:
                ring.mate_short(p, k)

    def arrive(ring, k, last, pieces=None):
        for p in pieces or range(len(ring.pieces)):
            ring.step_long(p, k, forward=not last)
            if not last:
                ring.step_short(p, k, forward=k < far - 1)

    def ring_steps(rings, body, before_last):
        def step(k, _):
            with jax.named_scope("arrive"):
                for ring in rings:
                    arrive(ring, k, False)
            with jax.named_scope("mates"):
                for ring in rings:
                    mates(ring, k, False)
            with jax.named_scope("compute"):
                four(k, body)
            return 0
        lax.fori_loop(1, far, step, 0)
        with jax.named_scope("before_last"):
            before_last()
        with jax.named_scope("arrive_last"):
            for ring in rings:
                arrive(ring, far, True)
        with jax.named_scope("mates_last"):
            for ring in rings:
                mates(ring, far, True)
        with jax.named_scope("compute_last"):
            pair(far, body)

    for p in range(2):
        ring_a.mate_own(p)
    pair(0, mlp_rows)
    ring_steps([ring_a], mlp_rows, lambda: ring_d.start_own(0))

    def finish_mlp(i, _):
        rows = pl.ds(pl.multiple_of(i * 64, 64), 64)
        t = x2[rows] - acc0[rows]
        x2[rows] = t
        xb[me, 0, rows] = (t * inv_rms(t)).astype(BF16)
        g = dyo[rows] + rms_back(x1[rows], acc1[rows])
        dyo[rows] = g
        xb[me, 1, rows] = g.astype(BF16)
        return 0

    with jax.named_scope("finish_mlp"):
        lax.fori_loop(0, toks // 64, finish_mlp, 0)
    ring_b.start_own(0)
    ring_b.start_own(1)

    with jax.named_scope("drain_a"):
        ring_a.drain()
    xa[me, 0] = uc[0]
    xa[me, 1] = uc[1]
    for dev in (pc.long_dev, pc.short_dev, pc.mate):
        pl.semaphore_signal(free_sem, inc=1, device_id={"tp": dev}, device_id_type=MESH)

    lane = lax.broadcasted_iota(jnp.int32, (toks, 4 * dim), 1)

    def project(d):
        w = w4[me, 0]
        stage[d] = jnp.where(lane < dim, dot_nt(xb[d, 1], w), dot_nt(xb[d, 0], w)).astype(BF16)

    for p in range(2):
        ring_b.mate_own(p)
    ring_d.mate_own(0)
    pair(0, project)

    def send_uc():
        pl.semaphore_wait(free_sem, 3)
        for p in range(2):
            ring_c.start_own(p)

    ring_steps([ring_d, ring_b], project, send_uc)

    full = n_dev * own
    low = lax.broadcasted_iota(jnp.int32, (full, 2 * dim), 1) < dim
    none = jnp.zeros((full, 2 * dim), BF16)

    def attend(block):
        left, right = block[:, :2 * dim], block[:, 2 * dim:]
        scores = dot_nt(jnp.where(low, none, left), right) * scale
        ex = jnp.exp(scores - jnp.max(scores, axis=-1, keepdims=True))
        prob = ex / jnp.sum(ex, axis=-1, keepdims=True)
        prob_b = prob.astype(BF16)
        d_prob = dot_nt(jnp.where(low, left, none), right)
        d_s = (prob * (d_prob - jnp.sum(d_prob * prob, axis=-1, keepdims=True)) * scale).astype(BF16)
        out_l = jnp.where(low, dot_nn(prob_b, right), dot_nn(d_s, right))
        out_r = jnp.where(low, dot_tn(prob_b, left), dot_tn(d_s, left))
        return out_l, out_r

    mine = pl.ds(pl.multiple_of(me * own, own), own)
    uc[0] = xb[:, 0, mine].reshape(full, hidden)
    uc[1] = xb[:, 1, mine].reshape(full, hidden)
    acc0[...] = jnp.zeros_like(acc0)

    def two_heads(i, _):
        o_pair, du = [], None
        for j in range(2):
            w = w4[2 * i + j, 0]
            block = jnp.where(lane < dim, dot_nt(uc[1], w), dot_nt(uc[0], w)).astype(BF16)
            out_l, out_r = attend(block)
            o_pair.append(out_l)
            out = jnp.concatenate([out_l, out_r], axis=1)
            part = dot_nn(jnp.where(lane < dim, 0.0, out).astype(BF16), w)
            du = part if du is None else du + part
        acc0[...] += du
        o_out[:, pl.ds(pl.multiple_of(i * 2 * dim, 2 * dim), 2 * dim)] = jnp.where(
            low, o_pair[0], pltpu.roll(o_pair[1], dim, axis=1)).astype(BF16)
        return 0

    n_pair = n_dev // 2
    with jax.named_scope("own_seq"):
        lax.fori_loop(0, n_pair // 2, two_heads, 0)
    with jax.named_scope("arrive_c1"):
        arrive(ring_c, 1, False)
    with jax.named_scope("own_seq"):
        lax.fori_loop(n_pair // 2, n_pair, two_heads, 0)

    def back(src_buf, dst_buf, i, hop):
        dev = lax.rem(me + hop, n_dev)
        theirs = pl.ds(pl.multiple_of(dev * own, own), own)
        return pltpu.make_async_remote_copy(
            src_ref=src_buf.at[theirs], dst_ref=dst_buf.at[mine],
            send_sem=all_send.at[i], recv_sem=all_recv.at[i],
            device_id={"tp": dev}, device_id_type=MESH)

    def all_back(buf, sem):
        ref = buf.at[pl.ds(0, (n_dev - 1) * own)]
        pltpu.make_async_copy(ref, ref, sem).wait()

    backs = [(o_out, o_in, 0), (acc0, du_in, 1)]
    for hop in range(1, n_dev):
        for args in backs:
            back(*args, hop).start()

    go[...] = jnp.zeros_like(go)
    gq[...] = jnp.zeros_like(gq)

    def own_head(s, _):
        rows = pl.ds(pl.multiple_of(s * own, own), own)
        out_l, out_r = attend(stage[:, rows].reshape(full, 4 * dim))
        turn = jnp.concatenate([out_l, out_r], axis=1).astype(BF16).T
        go[...] += dot_nn(turn[:dim], xb[:, 1, rows].reshape(full, hidden))
        g3 = dot_nn(turn[dim:], xb[:, 0, rows].reshape(full, hidden))
        gq[0] += g3[:dim]
        gq[2] += g3[dim:2 * dim]
        gq[1] += g3[2 * dim:]
        return 0

    gw2[...] = jnp.zeros_like(gw2)
    accw[...] = jnp.zeros_like(accw)

    def cols(ud, cd):
        h, da = activation(dot_nt(ud, w1t[...]), dot_nt(cd, w2own[...]))
        gw2[...] += dot_tn(h, cd)
        accw[...] += dot_tn(da, ud)

    def mlp_cols(d):
        cols(xa[d, 0], xa[d, 1])

    def finish():
        o_in[mine] = o_out[mine]
        du_in[mine] = acc0[mine]
        with jax.named_scope("wait_back"):
            all_back(o_in, all_recv.at[0])
            all_back(du_in, all_recv.at[1])
        x1[...] = x1[...] - dot_nn(o_in[...], w4[:, 0, pl.ds(0, dim)].reshape(n_dev * dim, hidden))

        def rows_out(i, _):
            rows = pl.ds(pl.multiple_of(i * 64, 64), 64)
            dx2[rows] = dx2[rows] + rms_back(x2[rows], du_in[rows])
            return 0

        lax.fori_loop(0, toks // 64, rows_out, 0)

    with jax.named_scope("own_cols"):
        for p in range(2):
            ring_c.mate_own(p)
        pair(0, mlp_cols)
    with jax.named_scope("cols_1"):
        mates(ring_c, 1, False)
        four(1, mlp_cols)
    with jax.named_scope("own_head"):
        lax.fori_loop(0, seqs // 2, own_head, 0)
    with jax.named_scope("arrive_c2"):
        arrive(ring_c, 2, False)
    with jax.named_scope("cols_2"):
        mates(ring_c, 2, False)
        four(2, mlp_cols)
    with jax.named_scope("own_head"):
        lax.fori_loop(seqs // 2, seqs, own_head, 0)
    with jax.named_scope("finish"):
        finish()
    for k in range(3, far):
        with jax.named_scope("arrive_c3"):
            arrive(ring_c, k, False)
        with jax.named_scope("cols_3"):
            mates(ring_c, k, False)
            four(k, mlp_cols)
    opposite = pl.ds(2 * lax.rem(pc.chip + far, pc.n_chip), 2)
    for p in range(2):
        with jax.named_scope("arrive_c4"):
            arrive(ring_c, far, True, (p,))
        with jax.named_scope("mates_c4"):
            mates(ring_c, far, True, (p,))
        with jax.named_scope("cols_4"):
            rows = pl.ds(p * half, half)
            cols(xa[opposite, 0, rows].reshape(toks, hidden), xa[opposite, 1, rows].reshape(toks, hidden))
    with jax.named_scope("tail"):
        ring_b.drain()
        ring_c.drain()
        ring_d.drain()
        all_back(o_in, all_send.at[0])
        all_back(du_in, all_send.at[1])


def writer(*refs):
    srcs, dsts, (turned, sem) = refs[:8], refs[8:16], refs[16:]
    copies = [pltpu.make_async_copy(turned if i == 6 else srcs[i], dsts[i], sem.at[i]) for i in range(8)]
    for i in (0, 1, 2, 3, 4, 5, 7):
        copies[i].start()
    turned[...] = srcs[6][...].T
    copies[6].start()
    for copy in copies:
        copy.wait()


def layer_backward(n_dev, y_one, y_two, dy_one, dy_two, wq, wo, wu, wd):
    seqs, own, hidden = y_one.shape
    n_loc, dim = wo.shape[0], wo.shape[1]
    toks = seqs * own
    cols = wu.shape[1]
    flat = lambda t: t.reshape(toks, hidden)
    any_spec = pl.BlockSpec(memory_space=pl.ANY)
    vmem = pl.BlockSpec(memory_space=pltpu.VMEM)
    far = n_dev // 4

    def ring_sems(p):
        dma = pltpu.SemaphoreType.DMA
        return (dma, dma((p, far)), dma((p, far - 1)), dma((p, 2 * far)))

    body = functools.partial(kernel, n_dev, seqs, own, dim, dim ** -0.5)

    def flat_body(*refs):
        main, sems = refs[:16 + 13], refs[16 + 13:]
        rings = [sems[4 * i:4 * i + 4] for i in range(4)]
        body(*main, *rings, *sems[16:])

    sems = [s for p in (2, 2, 2, 1) for s in ring_sems(p)]
    dma = pltpu.SemaphoreType.DMA
    shapes = [(toks, hidden)] * 4 + [(3, dim, hidden), (dim, hidden), (cols, hidden), (cols, hidden)]
    outs = pl.pallas_call(
        flat_body,
        name="reversible_block",
        out_shape=[pltpu.VMEM(shape, F32) for shape in shapes],
        in_specs=[any_spec] * 8,
        out_specs=[vmem] * 8,
        scratch_shapes=[
            pltpu.VMEM((n_dev, 2, toks, hidden), BF16),
            pltpu.VMEM((n_dev, 2, toks, hidden), BF16),
            pltpu.VMEM((n_dev, 1, 4 * dim, hidden), BF16),
            pltpu.VMEM((n_dev, toks, 4 * dim), BF16),
            pltpu.VMEM((2, toks, hidden), BF16),
            pltpu.VMEM((cols, hidden), BF16),
            pltpu.VMEM((cols, hidden), BF16),
            pltpu.VMEM((hidden, cols), BF16),
            pltpu.VMEM((toks, hidden), F32),
            pltpu.VMEM((toks, hidden), F32),
            pltpu.VMEM((toks, hidden), BF16),
            pltpu.VMEM((toks, hidden), BF16),
            pltpu.VMEM((toks, hidden), F32),
            *sems,
            dma((11,)),
            dma((2,)),
            dma((2,)),
            pltpu.SemaphoreType.REGULAR,
        ],
        compiler_params=pltpu.CompilerParams(collective_id=0, has_side_effects=True, vmem_limit_bytes=VMEM_GRANT),
    )(flat(y_one), flat(y_two), flat(dy_one), flat(dy_two), wu, wd, wo.reshape(n_loc * dim, hidden), wq.transpose(1, 2, 3, 0).reshape(3, dim, hidden))
    outs = pl.pallas_call(
        writer,
        name="write_results",
        out_shape=[jax.ShapeDtypeStruct((hidden, cols) if i == 6 else shape, F32) for i, shape in enumerate(shapes)],
        in_specs=[vmem] * 8,
        out_specs=[any_spec] * 8,
        scratch_shapes=[pltpu.VMEM((hidden, cols), F32), dma((8,))],
        compiler_params=pltpu.CompilerParams(vmem_limit_bytes=4 * 1024 * 1024),
    )(*[pltpu.with_memory_space_constraint(t, pltpu.VMEM) for t in outs])
    x_one, x_two, dx_one, dx_two, g_q, g_o, g_up, g_down = outs
    back = lambda t: t.reshape(y_one.shape)
    return back(x_one), back(x_two), back(dx_one), back(dx_two), g_q.reshape(n_loc, 3, dim, hidden).transpose(3, 0, 1, 2), g_o.reshape(wo.shape), g_up, g_down


def local_backward(n_dev, y_one, y_two, dy_one, dy_two, w_qkv, w_out, w_up, w_down):
    grads = []
    state = (y_one, y_two, dy_one, dy_two)
    for idx in reversed(range(w_qkv.shape[0])):
        res = layer_backward(n_dev, *state, w_qkv[idx], w_out[idx], w_up[idx], w_down[idx])
        state = res[:4]
        grads.append(res[4:])
    return state + tuple(jnp.stack(g[::-1]) for g in zip(*grads))


def solution(mesh):
    state_spec = P("dp", "tp", None)
    in_specs = (state_spec, state_spec, state_spec, state_spec, P(None, None, "tp", None, None), P(None, "tp", None, None), P(None, None, "tp"), P(None, "tp", None))
    out_specs = (state_spec, state_spec, state_spec, state_spec, P("dp", None, "tp", None, None), P("dp", "tp", None, None), P("dp", None, "tp"), P("dp", "tp", None))
    return jax.shard_map(functools.partial(local_backward, mesh.shape["tp"]), mesh=mesh, in_specs=in_specs, out_specs=out_specs, check_vma=False)
```
